16 devices in a mesh: dp: 4 (over y, z, core), tp: 4 (over x).
Axes of the slice: x: 4, y: 2, z: 1, core: 2. Of those that a mesh axis runs over, the one named last changes fastest.
The devices are a block of a 4x4x4 slice.
Arguments:
- x: bfloat16 [512, 12288], P('dp'), parts along dimension 0
- w_gate: bfloat16 [12288, 33792], P(None, 'tp')
- w_up: bfloat16 [12288, 33792], P(None, 'tp')
- w_down: bfloat16 [33792, 12288], P('tp')
Outputs:
- output: bfloat16 [512, 12288], P('dp'), parts along dimension 0
There are 4 independent parts. The reference program is written for one: setup_inputs(seed, part) draws one part's arguments, and reference() takes and returns one part's arrays. A program takes and returns all parts, laid end to end along the dimension named above; an argument that names none is the same for every part.
All inputs are finite; a program needn't handle non-finite values.
Results may differ from the reference program's by a relative error of at most 0.016.
Values are sent between devices in bfloat16 or wider.
A program may use at most 1.5 GiB of HBM per device.

```python
import jax
import jax.numpy as jnp

ROWS = 128
D = 12288
FF = 33792


def setup_inputs(seed: int = 0, part: int = 0) -> dict:
    kx, kg, ku, kd = jax.random.split(jax.random.key(seed), 4)
    drawn = {
        "x": jax.random.normal(jax.random.fold_in(kx, part), (ROWS, D), jnp.float32),
        "w_gate": jax.random.normal(kg, (D, FF), jnp.float32) * D**-0.5,
        "w_up": jax.random.normal(ku, (D, FF), jnp.float32) * D**-0.5,
        "w_down": jax.random.normal(kd, (FF, D), jnp.float32) * FF**-0.5,
    }
    return {k: v.astype(jnp.bfloat16) for k, v in drawn.items()}


def reference(x, w_gate, w_up, w_down):
    gate = jnp.dot(x, w_gate, preferred_element_type=jnp.float32)
    up = jnp.dot(x, w_up, preferred_element_type=jnp.float32)
    hidden = (jax.nn.silu(gate) * up).astype(jnp.bfloat16)
    return jnp.dot(hidden, w_down, preferred_element_type=jnp.float32).astype(jnp.bfloat16)
```

```python
import functools

import jax
import jax.numpy as jnp
from jax import lax
from jax.experimental import pallas as pl
from jax.experimental.pallas import tpu as pltpu
from jax.sharding import PartitionSpec as P

MESH = pl.DeviceIdType.MESH
SLOTS = 3
BN = 256
CN = 512
LAG_RS = 2
LAG_AG = 5
LAG_FW = 7
F32, BF16 = jnp.float32, jnp.bfloat16


def kernel(n, x_hbm, g_hbm, u_hbm, d_hbm, out, xb, hid, ring, accf, own, mid, s1_out, s1_in, s2_out, s2_in, fin,
           wsem, xsem, xsend, xrecv, hsend, hrecv, s1_send, s1_recv, s2_send, s2_recv, ag_send, near_recv, far_recv,
           sib_recv, fw_recv, fw_send):
    rows, depth = x_hbm.shape
    ff = d_hbm.shape[0]
    half = ff // 2
    full = half // BN
    rem = half - full * BN
    blocks = full + 1
    cols = out.shape[1] // 2
    chunks = cols // CN
    part = rows // n

    d, p = lax.axis_index("dp"), lax.axis_index("tp")
    c = lax.rem(d, 2)
    d0 = d - c
    sib = d0 + 1 - c
    right, left, opp = lax.rem(p + 1, n), lax.rem(p + n - 1, n), lax.rem(p + 2, n)
    fw_from = lax.rem(p + n - 1 + 2 * c, n)
    fw_to = lax.rem(p + n + 1 - 2 * c, n)

    def block_copies(b, first=False):
        s = 0 if first else lax.rem(b, SLOTS)
        w = rem if first else BN
        c0 = c * half if first else c * half + rem + (b - 1) * BN
        c0 = pl.multiple_of(c0, 128)
        return [
            pltpu.make_async_copy(h.at[:, pl.ds(c0, w)], ring.at[s, :, pl.ds(k * w, w)], wsem.at[s, k])
            for k, h in enumerate((g_hbm, u_hbm))
        ]

    def down_copy(t):
        s = lax.rem(t + blocks, SLOTS)
        c0 = pl.multiple_of(c * cols + t * CN, 128)
        return pltpu.make_async_copy(d_hbm.at[:, pl.ds(c0, CN)], ring.at[s, pl.ds(0, ff), :], wsem.at[s, 0])

    def start_block(b, first=False):
        for copy in block_copies(b, first):
            copy.start()

    def wait_block(b, first=False):
        for copy in block_copies(b, first):
            copy.wait()

    mine = pl.multiple_of(c * rows, rows)
    theirs = pl.multiple_of((1 - c) * rows, rows)
    x_copy = pltpu.make_async_copy(x_hbm, xb.at[pl.ds(mine, rows), :], xsem)
    x_copy.start()
    start_block(0, True)
    for b in range(1, SLOTS - 1):
        start_block(b)

    barrier = pltpu.get_barrier_semaphore()
    partners = [(sib, p)] + [(e, q) for e in (d, sib) for q in (left, right)]
    for dev in partners:
        pl.semaphore_signal(barrier, inc=1, device_id=dev, device_id_type=MESH)
    pl.semaphore_wait(barrier, len(partners))

    def remote(src, dst, send, recv, dev):
        return pltpu.make_async_remote_copy(
            src_ref=src, dst_ref=dst, send_sem=send, recv_sem=recv, device_id=dev, device_id_type=MESH)

    x_send = remote(x_hbm, xb.at[pl.ds(mine, rows), :], xsend, xrecv, (sib, p))
    x_send.start()
    x_copy.wait()
    remote(x_hbm, xb.at[pl.ds(theirs, rows), :], xsend, xrecv, (sib, p)).wait_recv()

    def act(r, w, c0):
        gate, up = r[:, :w], r[:, w:]
        hid[:, pl.ds(c0, w)] = (jax.nn.silu(gate) * up).astype(BF16)

    def send_hidden(c0, w):
        piece = hid.at[:, pl.ds(c0, w)]
        remote(piece, piece, hsend, hrecv, (sib, p)).start()

    def col(b):
        return pl.multiple_of(c * half + rem + (b - 1) * BN, 128)

    c_first = pl.multiple_of(c * half, 128)
    wait_block(0, True)
    start_block(SLOTS - 1)
    act(jnp.dot(xb[...], ring[0, :, : 2 * rem], preferred_element_type=F32), rem, c_first)

    def hidden_step(b, _):
        wait_block(b)
        ahead = b + SLOTS - 1

        @pl.when(ahead < blocks)
        def _():
            start_block(ahead)

        @pl.when(ahead >= blocks)
        def _():
            down_copy(ahead - blocks).start()

        @pl.when(b == 1)
        def _():
            send_hidden(c_first, rem)

        @pl.when(b > 1)
        def _():
            send_hidden(col(b - 1), BN)

        act(jnp.dot(xb[...], ring[lax.rem(b, SLOTS)], preferred_element_type=F32), BN, col(b))
        return 0

    lax.fori_loop(1, blocks, hidden_step, 0)

    own_half = pl.multiple_of(c * half, 128)
    sib_half = pl.multiple_of((1 - c) * half, 128)

    def stage(t):
        s1_out[t, 0] = accf[0, opp].astype(BF16)
        s1_out[t, 1] = accf[1, opp].astype(BF16)
        s2_out[t, 0, 1] = accf[1, right].astype(BF16)
        s2_out[t, 1, 0] = accf[0, left].astype(BF16)
        mid[t, 0] = accf[0, right]
        mid[t, 1] = accf[1, left]
        own[t, 0] = accf[0, p]
        own[t, 1] = accf[1, p]
        for g, q in ((0, right), (1, left)):
            remote(s1_out.at[t, g], s1_in.at[t, g], s1_send, s1_recv.at[t, g], (d, q)).start()

    def second_hop(t):
        for g, q in ((0, right), (1, left)):
            remote(s1_out.at[t, g], s1_in.at[t, g], s1_send, s1_recv.at[t, g], (d, q)).wait_recv()
            s2_out[t, g, g] = (mid[t, g] + s1_in[t, g].astype(F32)).astype(BF16)
        for g, q in ((0, right), (1, left)):
            remote(s2_out.at[t, g], s2_in.at[t, g], s2_send, s2_recv.at[t, g], (d, q)).start()

    def place(root, h, t):
        return out.at[pl.ds(pl.multiple_of(root * part, part), part), pl.ds(pl.multiple_of(h * cols + t * CN, 128), CN)]

    def finish(t):
        for g in (0, 1):
            remote(s2_out.at[t, g], s2_in.at[t, g], s2_send, s2_recv.at[t, g], (d, right)).wait_recv()
        for g in (0, 1):
            total = own[t, g] + s2_in[t, 0, g].astype(F32) + s2_in[t, 1, g].astype(F32)
            fin[t, g] = total.astype(BF16)
        for g in (0, 1):
            for q, ahead in ((right, g == 0), (left, g == 1)):
                sem = fw_recv.at[t, c] if ahead else near_recv
                remote(fin.at[t, g], place(p, c, t), ag_send, sem, (d0 + g, q)).start()
        remote(fin.at[t, 1 - c], place(p, c, t), ag_send, sib_recv, (sib, p)).start()
        r0 = pl.multiple_of(p * part, part)
        out[pl.ds(r0, part), pl.ds(pl.multiple_of(c * cols + t * CN, 128), CN)] = fin[t, c]

    def forward(t):
        for h in (0, 1):
            block = place(fw_from, h, t)
            remote(block, block, fw_send, fw_recv.at[t, h], (d, fw_to)).wait_recv()
            remote(block, block, fw_send, far_recv, (d, fw_to)).start()

    def behind(t):
        for lag, f in ((LAG_RS, second_hop), (LAG_AG, finish), (LAG_FW, forward)):
            @pl.when((t >= lag) & (t < chunks + lag))
            def _():
                f(t - lag)

    send_hidden(col(blocks - 1), BN)
    s0 = blocks % SLOTS
    down_copy(0).wait()
    down_copy(SLOTS - 1).start()
    r = jnp.dot(hid[:, pl.ds(own_half, half)], ring[s0, pl.ds(own_half, half), :], preferred_element_type=F32)
    accf[...] = r.reshape(accf.shape)
    theirs_h = hid.at[:, pl.ds(sib_half, half)]
    remote(theirs_h, theirs_h, hsend, hrecv, (sib, p)).wait_recv()
    r = jnp.dot(hid[:, pl.ds(sib_half, half)], ring[s0, pl.ds(sib_half, half), :], preferred_element_type=F32)
    accf[...] += r.reshape(accf.shape)
    stage(0)

    def down_step(t, _):
        down_copy(t).wait()

        @pl.when(t + SLOTS - 1 < chunks)
        def _():
            down_copy(t + SLOTS - 1).start()

        r = jnp.dot(hid[...], ring[lax.rem(t + blocks, SLOTS), pl.ds(0, ff), :], preferred_element_type=F32)
        accf[...] = r.reshape(accf.shape)
        stage(t)
        behind(t)
        return 0

    lax.fori_loop(1, chunks, down_step, 0)

    def drain_step(t, _):
        behind(t)
        return 0

    lax.fori_loop(chunks, chunks + LAG_FW, drain_step, 0)

    def row_block(q):
        return out.at[pl.ds(pl.multiple_of(q * part, part), part), :]

    near = row_block(fw_to)
    remote(near, near, ag_send, near_recv, (d, left)).wait_recv()
    far = row_block(opp)
    remote(far, far, ag_send, far_recv, (d, left)).wait_recv()
    sib_cols = out.at[pl.ds(pl.multiple_of(p * part, part), part), pl.ds(pl.multiple_of((1 - c) * cols, 128), cols)]
    remote(sib_cols, sib_cols, ag_send, sib_recv, (sib, p)).wait_recv()
    x_send.wait_send()
    mine_h = hid.at[:, pl.ds(own_half, half)]
    remote(mine_h, mine_h, hsend, hrecv, (sib, p)).wait_send()
    remote(s1_out, s1_in, s1_send, s1_recv.at[0, 0], (d, right)).wait_send()
    remote(s2_out, s2_in, s2_send, s2_recv.at[0, 0], (d, right)).wait_send()
    for _ in range(2):
        remote(fin, fin, ag_send, near_recv, (d, right)).wait_send()
    remote(sib_cols, sib_cols, ag_send, sib_recv, (sib, p)).wait_send()
    remote(near, near, fw_send, far_recv, (d, left)).wait_send()


def solution(mesh):
    n = mesh.shape["tp"]

    def step(x, w_gate, w_up, w_down):
        rows, depth = x.shape
        ff, width = w_down.shape
        cols, part = width // 2, rows // n
        chunks = cols // CN
        dma = pltpu.SemaphoreType.DMA
        flops = 2 * rows * (2 * depth * ff + ff * width)
        return pl.pallas_call(
            functools.partial(kernel, n),
            out_shape=jax.ShapeDtypeStruct((rows, width), BF16),
            in_specs=[pl.BlockSpec(memory_space=pl.ANY)] * 4,
            out_specs=pl.BlockSpec(memory_space=pltpu.VMEM),
            scratch_shapes=[
                pltpu.VMEM((2 * rows, depth), BF16),
                pltpu.VMEM((2 * rows, ff), BF16),
                pltpu.VMEM((SLOTS, depth, 2 * BN), BF16),
                pltpu.VMEM((2, n, part, CN), F32),
                pltpu.VMEM((chunks, 2, part, CN), F32),
                pltpu.VMEM((chunks, 2, part, CN), F32),
                pltpu.VMEM((chunks, 2, part, CN), BF16),
                pltpu.VMEM((chunks, 2, part, CN), BF16),
                pltpu.VMEM((chunks, 2, 2, part, CN), BF16),
                pltpu.VMEM((chunks, 2, 2, part, CN), BF16),
                pltpu.VMEM((chunks, 2, part, CN), BF16),
                dma((SLOTS, 2)), dma, dma, dma, dma, dma,
                dma, dma((chunks, 2)), dma, dma((chunks, 2)),
                dma, dma, dma, dma, dma((chunks, 2)), dma,
            ],
            compiler_params=pltpu.CompilerParams(
                collective_id=0, has_side_effects=True, vmem_limit_bytes=67043328),
            cost_estimate=pl.CostEstimate(
                flops=flops, bytes_accessed=3 * depth * ff, transcendentals=rows * ff),
        )(x, w_gate, w_up, w_down)

    return jax.shard_map(
        step,
        mesh=mesh,
        in_specs=(P("dp", None), P(None, "tp"), P(None, "tp"), P("tp", None)),
        out_specs=P("dp", None),
        check_vma=False,
    )
```

```python
import functools

import jax
import jax.numpy as jnp
from jax import lax
from jax.experimental import pallas as pl
from jax.experimental.pallas import tpu as pltpu
from jax.sharding import PartitionSpec as P

MESH = pl.DeviceIdType.MESH
SLOTS = 3
BN = 256
CN = 512
LAG_RS = 1
LAG_AG = 3
LAG_FW = 5
F32, BF16 = jnp.float32, jnp.bfloat16


def kernel(n, x_hbm, g_hbm, u_hbm, d_hbm, out, xb, hid, ring, accf, own, mid, s1_out, s1_in, s2_out, s2_in, fin,
           wsem, xsem, xsend, xrecv, hsend, hrecv, s1_send, s1_recv, s2_send, s2_recv, ag_send, near_recv, far_recv,
           sib_recv, fw_recv, fw_send):
    rows, depth = x_hbm.shape
    ff = d_hbm.shape[0]
    half = ff // 2
    full = half // BN
    rem = half - full * BN
    blocks = full + 1
    cols = out.shape[1] // 2
    chunks = cols // CN
    part = rows // n

    d, p = lax.axis_index("dp"), lax.axis_index("tp")
    c = lax.rem(d, 2)
    d0 = d - c
    sib = d0 + 1 - c
    right, left, opp = lax.rem(p + 1, n), lax.rem(p + n - 1, n), lax.rem(p + 2, n)
    fw_from = lax.rem(p + n - 1 + 2 * c, n)
    fw_to = lax.rem(p + n + 1 - 2 * c, n)

    def block_copies(b, first=False):
        s = 0 if first else lax.rem(b, SLOTS)
        w = rem if first else BN
        c0 = c * half if first else c * half + rem + (b - 1) * BN
        c0 = pl.multiple_of(c0, 128)
        return [
            pltpu.make_async_copy(h.at[:, pl.ds(c0, w)], ring.at[s, :, pl.ds(k * w, w)], wsem.at[s, k])
            for k, h in enumerate((g_hbm, u_hbm))
        ]

    def down_copy(t):
        s = lax.rem(t + blocks, SLOTS)
        c0 = pl.multiple_of(c * cols + t * CN, 128)
        return pltpu.make_async_copy(d_hbm.at[:, pl.ds(c0, CN)], ring.at[s, pl.ds(0, ff), :], wsem.at[s, 0])

    def start_block(b, first=False):
        for copy in block_copies(b, first):
            copy.start()

    def wait_block(b, first=False):
        for copy in block_copies(b, first):
            copy.wait()

    mine = pl.multiple_of(c * rows, rows)
    theirs = pl.multiple_of((1 - c) * rows, rows)
    x_copy = pltpu.make_async_copy(x_hbm, xb.at[pl.ds(mine, rows), :], xsem)
    x_copy.start()
    start_block(0, True)
    for b in range(1, SLOTS - 1):
        start_block(b)

    barrier = pltpu.get_barrier_semaphore()
    partners = [(sib, p)] + [(e, q) for e in (d, sib) for q in (left, right)]
    for dev in partners:
        pl.semaphore_signal(barrier, inc=1, device_id=dev, device_id_type=MESH)
    pl.semaphore_wait(barrier, len(partners))

    def remote(src, dst, send, recv, dev):
        return pltpu.make_async_remote_copy(
            src_ref=src, dst_ref=dst, send_sem=send, recv_sem=recv, device_id=dev, device_id_type=MESH)

    x_send = remote(x_hbm, xb.at[pl.ds(mine, rows), :], xsend, xrecv, (sib, p))
    x_send.start()
    x_copy.wait()
    remote(x_hbm, xb.at[pl.ds(theirs, rows), :], xsend, xrecv, (sib, p)).wait_recv()

    def act(r, w, c0):
        gate, up = r[:, :w], r[:, w:]
        hid[:, pl.ds(c0, w)] = (jax.nn.silu(gate) * up).astype(BF16)

    def send_hidden(c0, w):
        piece = hid.at[:, pl.ds(c0, w)]
        remote(piece, piece, hsend, hrecv, (sib, p)).start()

    def col(b):
        return pl.multiple_of(c * half + rem + (b - 1) * BN, 128)

    c_first = pl.multiple_of(c * half, 128)
    wait_block(0, True)
    start_block(SLOTS - 1)
    act(jnp.dot(xb[...], ring[0, :, : 2 * rem], preferred_element_type=F32), rem, c_first)

    def hidden_step(b, _):
        wait_block(b)
        ahead = b + SLOTS - 1

        @pl.when(ahead < blocks)
        def _():
            start_block(ahead)

        @pl.when(ahead >= blocks)
        def _():
            down_copy(ahead - blocks).start()

        @pl.when(b == 1)
        def _():
            send_hidden(c_first, rem)

        @pl.when(b > 1)
        def _():
            send_hidden(col(b - 1), BN)

        act(jnp.dot(xb[...], ring[lax.rem(b, SLOTS)], preferred_element_type=F32), BN, col(b))
        return 0

    lax.fori_loop(1, blocks, hidden_step, 0)

    own_half = pl.multiple_of(c * half, 128)
    sib_half = pl.multiple_of((1 - c) * half, 128)

    def stage(t):
        s1_out[t, 0] = accf[0, opp].astype(BF16)
        s1_out[t, 1] = accf[1, opp].astype(BF16)
        s2_out[t, 0, 1] = accf[1, right].astype(BF16)
        s2_out[t, 1, 0] = accf[0, left].astype(BF16)
        mid[t, 0] = accf[0, right]
        mid[t, 1] = accf[1, left]
        own[t, 0] = accf[0, p]
        own[t, 1] = accf[1, p]
        for g, q in ((0, right), (1, left)):
            remote(s1_out.at[t, g], s1_in.at[t, g], s1_send, s1_recv.at[t, g], (d, q)).start()

    def second_hop(t):
        for g, q in ((0, right), (1, left)):
            remote(s1_out.at[t, g], s1_in.at[t, g], s1_send, s1_recv.at[t, g], (d, q)).wait_recv()
            s2_out[t, g, g] = (mid[t, g] + s1_in[t, g].astype(F32)).astype(BF16)
        for g, q in ((0, right), (1, left)):
            remote(s2_out.at[t, g], s2_in.at[t, g], s2_send, s2_recv.at[t, g], (d, q)).start()

    def place(root, h, t):
        return out.at[pl.ds(pl.multiple_of(root * part, part), part), pl.ds(pl.multiple_of(h * cols + t * CN, 128), CN)]

    def finish(t):
        for g in (0, 1):
            remote(s2_out.at[t, g], s2_in.at[t, g], s2_send, s2_recv.at[t, g], (d, right)).wait_recv()
        for g in (0, 1):
            total = own[t, g] + s2_in[t, 0, g].astype(F32) + s2_in[t, 1, g].astype(F32)
            fin[t, g] = total.astype(BF16)
        for g in (0, 1):
            for q, ahead in ((right, g == 0), (left, g == 1)):
                sem = fw_recv.at[t, c] if ahead else near_recv
                remote(fin.at[t, g], place(p, c, t), ag_send, sem, (d0 + g, q)).start()
        remote(fin.at[t, 1 - c], place(p, c, t), ag_send, sib_recv, (sib, p)).start()
        r0 = pl.multiple_of(p * part, part)
        out[pl.ds(r0, part), pl.ds(pl.multiple_of(c * cols + t * CN, 128), CN)] = fin[t, c]

    def forward(t):
        for h in (0, 1):
            block = place(fw_from, h, t)
            remote(block, block, fw_send, fw_recv.at[t, h], (d, fw_to)).wait_recv()
            remote(block, block, fw_send, far_recv, (d, fw_to)).start()

    def behind(t):
        for lag, f in ((LAG_RS, second_hop), (LAG_AG, finish), (LAG_FW, forward)):
            @pl.when((t >= lag) & (t < chunks + lag))
            def _():
                f(t - lag)

    send_hidden(col(blocks - 1), BN)
    s0 = blocks % SLOTS
    down_copy(0).wait()
    down_copy(SLOTS - 1).start()
    r = jnp.dot(hid[:, pl.ds(own_half, half)], ring[s0, pl.ds(own_half, half), :], preferred_element_type=F32)
    accf[...] = r.reshape(accf.shape)
    theirs_h = hid.at[:, pl.ds(sib_half, half)]
    remote(theirs_h, theirs_h, hsend, hrecv, (sib, p)).wait_recv()
    r = jnp.dot(hid[:, pl.ds(sib_half, half)], ring[s0, pl.ds(sib_half, half), :], preferred_element_type=F32)
    accf[...] += r.reshape(accf.shape)
    stage(0)

    def down_step(t, _):
        down_copy(t).wait()

        @pl.when(t + SLOTS - 1 < chunks)
        def _():
            down_copy(t + SLOTS - 1).start()

        r = jnp.dot(hid[...], ring[lax.rem(t + blocks, SLOTS), pl.ds(0, ff), :], preferred_element_type=F32)
        accf[...] = r.reshape(accf.shape)
        stage(t)
        behind(t)
        return 0

    lax.fori_loop(1, chunks, down_step, 0)

    def drain_step(t, _):
        behind(t)
        return 0

    lax.fori_loop(chunks, chunks + LAG_FW, drain_step, 0)

    def row_block(q):
        return out.at[pl.ds(pl.multiple_of(q * part, part), part), :]

    near = row_block(fw_to)
    remote(near, near, ag_send, near_recv, (d, left)).wait_recv()
    far = row_block(opp)
    remote(far, far, ag_send, far_recv, (d, left)).wait_recv()
    sib_cols = out.at[pl.ds(pl.multiple_of(p * part, part), part), pl.ds(pl.multiple_of((1 - c) * cols, 128), cols)]
    remote(sib_cols, sib_cols, ag_send, sib_recv, (sib, p)).wait_recv()
    x_send.wait_send()
    mine_h = hid.at[:, pl.ds(own_half, half)]
    remote(mine_h, mine_h, hsend, hrecv, (sib, p)).wait_send()
    remote(s1_out, s1_in, s1_send, s1_recv.at[0, 0], (d, right)).wait_send()
    remote(s2_out, s2_in, s2_send, s2_recv.at[0, 0], (d, right)).wait_send()
    for _ in range(2):
        remote(fin, fin, ag_send, near_recv, (d, right)).wait_send()
    remote(sib_cols, sib_cols, ag_send, sib_recv, (sib, p)).wait_send()
    remote(near, near, fw_send, far_recv, (d, left)).wait_send()


def solution(mesh):
    n = mesh.shape["tp"]

    def step(x, w_gate, w_up, w_down):
        rows, depth = x.shape
        ff, width = w_down.shape
        cols, part = width // 2, rows // n
        chunks = cols // CN
        dma = pltpu.SemaphoreType.DMA
        flops = 2 * rows * (2 * depth * ff + ff * width)
        return pl.pallas_call(
            functools.partial(kernel, n),
            out_shape=pltpu.VMEM((rows, width), BF16),
            in_specs=[pl.BlockSpec(memory_space=pl.ANY)] * 4,
            out_specs=pl.BlockSpec(memory_space=pltpu.VMEM),
            scratch_shapes=[
                pltpu.VMEM((2 * rows, depth), BF16),
                pltpu.VMEM((2 * rows, ff), BF16),
                pltpu.VMEM((SLOTS, depth, 2 * BN), BF16),
                pltpu.VMEM((2, n, part, CN), F32),
                pltpu.VMEM((chunks, 2, part, CN), F32),
                pltpu.VMEM((chunks, 2, part, CN), F32),
                pltpu.VMEM((chunks, 2, part, CN), BF16),
                pltpu.VMEM((chunks, 2, part, CN), BF16),
                pltpu.VMEM((chunks, 2, 2, part, CN), BF16),
                pltpu.VMEM((chunks, 2, 2, part, CN), BF16),
                pltpu.VMEM((chunks, 2, part, CN), BF16),
                dma((SLOTS, 2)), dma, dma, dma, dma, dma,
                dma, dma((chunks, 2)), dma, dma((chunks, 2)),
                dma, dma, dma, dma, dma((chunks, 2)), dma,
            ],
            compiler_params=pltpu.CompilerParams(
                collective_id=0, has_side_effects=True, vmem_limit_bytes=63700000),
            cost_estimate=pl.CostEstimate(
                flops=flops, bytes_accessed=3 * depth * ff, transcendentals=rows * ff),
        )(x, w_gate, w_up, w_down)

    return jax.shard_map(
        step,
        mesh=mesh,
        in_specs=(P("dp", None), P(None, "tp"), P(None, "tp"), P("tp", None)),
        out_specs=P("dp", None),
        check_vma=False,
    )
```

```python
import functools

import jax
import jax.numpy as jnp
from jax import lax
from jax.experimental import pallas as pl
from jax.experimental.pallas import tpu as pltpu
from jax.sharding import PartitionSpec as P

MESH = pl.DeviceIdType.MESH
SLOTS = 3
BN = 256
XP = 4
CN = 512
LAG_RS = 1
LAG_AG = 3
LAG_FW = 6
F32, BF16 = jnp.float32, jnp.bfloat16


def kernel(n, x_hbm, g_hbm, u_hbm, d_hbm, out, xb, hid, ring, accf, own, mid, s1_out, s1_in, s2_out, s2_in, fin,
           wsem, xsem, xsend, xrecv, hsend, hrecv, s1_send, s1_recv, s2_send, s2_recv, ag_send, near_recv, far_recv,
           sib_recv, fw_recv, fw_send):
    rows, depth = x_hbm.shape
    ff = d_hbm.shape[0]
    half = ff // 2
    full = half // BN
    rem = half - full * BN
    blocks = full + 1
    cols = out.shape[1] // 2
    chunks = cols // CN
    part = rows // n

    d, p = lax.axis_index("dp"), lax.axis_index("tp")
    c = lax.rem(d, 2)
    d0 = d - c
    sib = d0 + 1 - c
    right, left, opp = lax.rem(p + 1, n), lax.rem(p + n - 1, n), lax.rem(p + 2, n)
    fw_from = lax.rem(p + n - 1 + 2 * c, n)
    fw_to = lax.rem(p + n + 1 - 2 * c, n)

    def block_copies(b, first=False):
        s = 0 if first else lax.rem(b, SLOTS)
        w = rem if first else BN
        c0 = c * half if first else c * half + rem + (b - 1) * BN
        c0 = pl.multiple_of(c0, 128)
        return [
            pltpu.make_async_copy(h.at[:, pl.ds(c0, w)], ring.at[s, :, pl.ds(k * w, w)], wsem.at[s, k])
            for k, h in enumerate((g_hbm, u_hbm))
        ]

    def down_copy(t):
        s = lax.rem(t + blocks, SLOTS)
        c0 = pl.multiple_of(c * cols + t * CN, 128)
        return pltpu.make_async_copy(d_hbm.at[:, pl.ds(c0, CN)], ring.at[s, pl.ds(0, ff), :], wsem.at[s, 0])

    def start_block(b, first=False):
        for copy in block_copies(b, first):
            copy.start()

    def wait_block(b, first=False):
        for copy in block_copies(b, first):
            copy.wait()

    mine = pl.multiple_of(c * rows, rows)
    theirs = pl.multiple_of((1 - c) * rows, rows)
    cut = depth // XP

    def x_copy(i):
        piece = pl.ds(i * cut, cut)
        return pltpu.make_async_copy(x_hbm.at[:, piece], xb.at[pl.ds(mine, rows), piece], xsem.at[i])

    for i in range(XP):
        x_copy(i).start()
    start_block(0, True)
    for b in range(1, SLOTS - 1):
        start_block(b)

    barrier = pltpu.get_barrier_semaphore()
    partners = [(sib, p)] + [(e, q) for e in (d, sib) for q in (left, right)]
    for dev in partners:
        pl.semaphore_signal(barrier, inc=1, device_id=dev, device_id_type=MESH)
    pl.semaphore_wait(barrier, len(partners))

    def remote(src, dst, send, recv, dev):
        return pltpu.make_async_remote_copy(
            src_ref=src, dst_ref=dst, send_sem=send, recv_sem=recv, device_id=dev, device_id_type=MESH)

    def x_send(i, base):
        piece = xb.at[pl.ds(base, rows), pl.ds(i * cut, cut)]
        return remote(piece, piece, xsend.at[i], xrecv.at[i], (sib, p))

    for i in range(XP):
        x_copy(i).wait()
        x_send(i, mine).start()

    def act(r, w, c0):
        gate, up = r[:, :w], r[:, w:]
        hid[:, pl.ds(c0, w)] = (jax.nn.silu(gate) * up).astype(BF16)

    def send_hidden(c0, w):
        piece = hid.at[:, pl.ds(c0, w)]
        remote(piece, piece, hsend, hrecv, (sib, p)).start()

    def col(b):
        return pl.multiple_of(c * half + rem + (b - 1) * BN, 128)

    c_first = pl.multiple_of(c * half, 128)
    wait_block(0, True)
    start_block(SLOTS - 1)
    total = jnp.zeros((2 * rows, 2 * rem), F32)
    for i in range(XP):
        x_send(i, theirs).wait_recv()
        piece = slice(i * cut, (i + 1) * cut)
        total += jnp.dot(xb[:, piece], ring[0, piece, : 2 * rem], preferred_element_type=F32)
    act(total, rem, c_first)

    def hidden_step(b, _):
        wait_block(b)
        ahead = b + SLOTS - 1

        @pl.when(ahead < blocks)
        def _():
            start_block(ahead)

        @pl.when(ahead >= blocks)
        def _():
            down_copy(ahead - blocks).start()

        @pl.when(b == 1)
        def _():
            send_hidden(c_first, rem)

        @pl.when(b > 1)
        def _():
            send_hidden(col(b - 1), BN)

        act(jnp.dot(xb[...], ring[lax.rem(b, SLOTS)], preferred_element_type=F32), BN, col(b))
        return 0

    lax.fori_loop(1, blocks, hidden_step, 0)

    own_half = pl.multiple_of(c * half, 128)
    sib_half = pl.multiple_of((1 - c) * half, 128)

    def stage(t):
        s1_out[t, 0] = accf[0, opp].astype(BF16)
        s1_out[t, 1] = accf[1, opp].astype(BF16)
        s2_out[t, 0, 1] = accf[1, right].astype(BF16)
        s2_out[t, 1, 0] = accf[0, left].astype(BF16)
        mid[t, 0] = accf[0, right]
        mid[t, 1] = accf[1, left]
        own[t, 0] = accf[0, p]
        own[t, 1] = accf[1, p]
        for g, q in ((0, right), (1, left)):
            remote(s1_out.at[t, g], s1_in.at[t, g], s1_send, s1_recv.at[t, g], (d, q)).start()

    def second_hop(t):
        for g, q in ((0, right), (1, left)):
            remote(s1_out.at[t, g], s1_in.at[t, g], s1_send, s1_recv.at[t, g], (d, q)).wait_recv()
            s2_out[t, g, g] = (mid[t, g] + s1_in[t, g].astype(F32)).astype(BF16)
        for g, q in ((0, right), (1, left)):
            remote(s2_out.at[t, g], s2_in.at[t, g], s2_send, s2_recv.at[t, g], (d, q)).start()

    def place(root, h, t):
        return out.at[pl.ds(pl.multiple_of(root * part, part), part), pl.ds(pl.multiple_of(h * cols + t * CN, 128), CN)]

    def finish(t):
        for g in (0, 1):
            remote(s2_out.at[t, g], s2_in.at[t, g], s2_send, s2_recv.at[t, g], (d, right)).wait_recv()
        for g in (0, 1):
            total = own[t, g] + s2_in[t, 0, g].astype(F32) + s2_in[t, 1, g].astype(F32)
            fin[t, g] = total.astype(BF16)
        for g, q in ((0, right), (1, left)):
            remote(fin.at[t, g], place(p, c, t), ag_send, fw_recv.at[t, c], (d0 + g, q)).start()
        for g, q in ((1, right), (0, left)):
            remote(fin.at[t, g], place(p, c, t), ag_send, near_recv, (d0 + g, q)).start()
        remote(fin.at[t, 1 - c], place(p, c, t), ag_send, sib_recv, (sib, p)).start()
        r0 = pl.multiple_of(p * part, part)
        out[pl.ds(r0, part), pl.ds(pl.multiple_of(c * cols + t * CN, 128), CN)] = fin[t, c]

    def forward(t):
        for h in (0, 1):
            block = place(fw_from, h, t)
            remote(block, block, fw_send, fw_recv.at[t, h], (d, fw_to)).wait_recv()
            remote(block, block, fw_send, far_recv, (d, fw_to)).start()

    def behind(t):
        for lag, f in ((LAG_RS, second_hop), (LAG_AG, finish), (LAG_FW, forward)):
            @pl.when((t >= lag) & (t < chunks + lag))
            def _():
                f(t - lag)

    send_hidden(col(blocks - 1), BN)
    s0 = blocks % SLOTS
    down_copy(0).wait()
    down_copy(SLOTS - 1).start()
    r = jnp.dot(hid[:, pl.ds(own_half, half)], ring[s0, pl.ds(own_half, half), :], preferred_element_type=F32)
    accf[...] = r.reshape(accf.shape)
    theirs_h = hid.at[:, pl.ds(sib_half, half)]
    remote(theirs_h, theirs_h, hsend, hrecv, (sib, p)).wait_recv()
    r = jnp.dot(hid[:, pl.ds(sib_half, half)], ring[s0, pl.ds(sib_half, half), :], preferred_element_type=F32)
    accf[...] += r.reshape(accf.shape)
    stage(0)

    def down_step(t, _):
        down_copy(t).wait()

        @pl.when(t + SLOTS - 1 < chunks)
        def _():
            down_copy(t + SLOTS - 1).start()

        r = jnp.dot(hid[...], ring[lax.rem(t + blocks, SLOTS), pl.ds(0, ff), :], preferred_element_type=F32)
        accf[...] = r.reshape(accf.shape)
        stage(t)
        behind(t)
        return 0

    lax.fori_loop(1, chunks, down_step, 0)

    def drain_step(t, _):
        behind(t)
        return 0

    lax.fori_loop(chunks, chunks + LAG_FW, drain_step, 0)

    def row_block(q):
        return out.at[pl.ds(pl.multiple_of(q * part, part), part), :]

    near = row_block(fw_to)
    remote(near, near, ag_send, near_recv, (d, left)).wait_recv()
    far = row_block(opp)
    remote(far, far, ag_send, far_recv, (d, left)).wait_recv()
    sib_cols = out.at[pl.ds(pl.multiple_of(p * part, part), part), pl.ds(pl.multiple_of((1 - c) * cols, 128), cols)]
    remote(sib_cols, sib_cols, ag_send, sib_recv, (sib, p)).wait_recv()
    for i in range(XP):
        x_send(i, mine).wait_send()
    mine_h = hid.at[:, pl.ds(own_half, half)]
    remote(mine_h, mine_h, hsend, hrecv, (sib, p)).wait_send()
    remote(s1_out, s1_in, s1_send, s1_recv.at[0, 0], (d, right)).wait_send()
    remote(s2_out, s2_in, s2_send, s2_recv.at[0, 0], (d, right)).wait_send()
    for _ in range(2):
        remote(fin, fin, ag_send, near_recv, (d, right)).wait_send()
    remote(sib_cols, sib_cols, ag_send, sib_recv, (sib, p)).wait_send()
    remote(near, near, fw_send, far_recv, (d, left)).wait_send()


def solution(mesh):
    n = mesh.shape["tp"]

    def step(x, w_gate, w_up, w_down):
        rows, depth = x.shape
        ff, width = w_down.shape
        cols, part = width // 2, rows // n
        chunks = cols // CN
        dma = pltpu.SemaphoreType.DMA
        flops = 2 * rows * (2 * depth * ff + ff * width)
        return pl.pallas_call(
            functools.partial(kernel, n),
            out_shape=pltpu.VMEM((rows, width), BF16),
            in_specs=[pl.BlockSpec(memory_space=pl.ANY)] * 4,
            out_specs=pl.BlockSpec(memory_space=pltpu.VMEM),
            scratch_shapes=[
                pltpu.VMEM((2 * rows, depth), BF16),
                pltpu.VMEM((2 * rows, ff), BF16),
                pltpu.VMEM((SLOTS, depth, 2 * BN), BF16),
                pltpu.VMEM((2, n, part, CN), F32),
                pltpu.VMEM((chunks, 2, part, CN), F32),
                pltpu.VMEM((chunks, 2, part, CN), F32),
                pltpu.VMEM((chunks, 2, part, CN), BF16),
                pltpu.VMEM((chunks, 2, part, CN), BF16),
                pltpu.VMEM((chunks, 2, 2, part, CN), BF16),
                pltpu.VMEM((chunks, 2, 2, part, CN), BF16),
                pltpu.VMEM((chunks, 2, part, CN), BF16),
                dma((SLOTS, 2)), dma((XP,)), dma((XP,)), dma((XP,)), dma, dma,
                dma, dma((chunks, 2)), dma, dma((chunks, 2)),
                dma, dma, dma, dma, dma((chunks, 2)), dma,
            ],
            compiler_params=pltpu.CompilerParams(
                collective_id=0, has_side_effects=True, vmem_limit_bytes=63700000),
            cost_estimate=pl.CostEstimate(
                flops=flops, bytes_accessed=3 * depth * ff, transcendentals=rows * ff),
        )(x, w_gate, w_up, w_down)

    return jax.shard_map(
        step,
        mesh=mesh,
        in_specs=(P("dp", None), P(None, "tp"), P(None, "tp"), P("tp", None)),
        out_specs=P("dp", None),
        check_vma=False,
    )
```
